128 devices in a mesh: ga: 128 (over z, y, x, core).
Axes of the slice: x: 4, y: 4, z: 4, core: 2. Of those that a mesh axis runs over, the one named last changes fastest.
Arguments:
- text_states: bfloat16 [2048, 640], P('ga')
- text_proj: bfloat16 [640, 640], replicated
- gallery: bfloat16 [262144, 640], P('ga')
- logit_scale: float32 [1], replicated
Outputs:
- output 1: bfloat16 [2048, 262144], P(None, 'ga')
- output 2: float32 [2048], replicated
All inputs are finite; a program needn't handle non-finite values.
Results may differ from the reference program's by a relative error of at most 0.001.
Values are sent between devices in bfloat16 or wider.
A program may use at most 1 GiB of HBM per device.

```python
import jax
import jax.numpy as jnp
from jax import lax

QUERIES = 2048
GALLERY = 262144
WT = 640
EMB = 640
QBLOCK = 16


def setup_inputs(seed: int = 0) -> dict:
    base_key = jax.random.key(seed)
    k_text, k_proj, k_noise, k_dirs, k_scale = jax.random.split(base_key, 5)
    text_states = jax.random.normal(k_text, (QUERIES, WT), jnp.float32)
    text_proj = jax.random.normal(k_proj, (WT, EMB), jnp.float32) * WT ** -0.5
    anchors = jax.random.normal(k_dirs, (2, EMB), jnp.float32)
    anchors = anchors / jnp.sqrt(jnp.sum(anchors * anchors, axis=1, keepdims=True))
    angles = jnp.pi * jnp.arange(GALLERY, dtype=jnp.float32) / GALLERY
    gallery = (jax.random.normal(k_noise, (GALLERY, EMB), jnp.float32) * EMB ** -0.5
               + jnp.cos(angles)[:, None] * anchors[0] + jnp.sin(angles)[:, None] * anchors[1])
    gallery = gallery / jnp.sqrt(jnp.sum(gallery * gallery, axis=1, keepdims=True))
    logit_scale = (0.5 * jnp.log(2.0 * EMB) + jnp.log(1.5)
                   + jax.random.uniform(k_scale, (1,), jnp.float32, -0.2, 0.2)).astype(jnp.float32)
    return {
        "text_states": text_states.astype(jnp.bfloat16),
        "text_proj": text_proj.astype(jnp.bfloat16),
        "gallery": gallery.astype(jnp.bfloat16),
        "logit_scale": logit_scale,
    }


def reference(text_states, text_proj, gallery, logit_scale):
    proj_out = jnp.dot(text_states, text_proj, preferred_element_type=jnp.float32)
    unit_q = proj_out / jnp.sqrt(jnp.sum(proj_out * proj_out, axis=1, keepdims=True))
    query_emb = unit_q.astype(jnp.bfloat16)
    logit_mult = jnp.exp(logit_scale[0])
    positions = jnp.arange(GALLERY, dtype=jnp.float32) / GALLERY
    blocks = query_emb.reshape(QUERIES // QBLOCK, QBLOCK, EMB)

    def score_block(query_block):
        scores = logit_mult * jnp.dot(query_block, gallery.T, preferred_element_type=jnp.float32)
        row_max = jnp.max(scores, axis=1, keepdims=True)
        exp_vals = jnp.exp(scores - row_max)
        prob_vals = exp_vals / jnp.sum(exp_vals, axis=1, keepdims=True)
        return prob_vals.astype(jnp.bfloat16), jnp.sum(prob_vals * positions, axis=1)

    prob_blocks, rank_blocks = lax.map(score_block, blocks)
    return prob_blocks.reshape(QUERIES, GALLERY), rank_blocks.reshape(QUERIES)
```

```python
import jax
import jax.numpy as jnp
from jax import lax
from jax.experimental import pallas as pl
from jax.experimental.pallas import tpu as pltpu
from jax.sharding import PartitionSpec as P

MESH = pl.DeviceIdType.MESH
LOG2E = 1.4426950408889634
Z, Y, X = 0, 1, 2
ROUTES = (((X, Y, Z), 0, 256), ((Y, Z, X), 256, 256), ((Z, X, Y), 512, 128))
CHUNK = 256


def device_of(pos, core):
    return ((pos[0] * 4 + pos[1]) * 4 + pos[2]) * 2 + core


def kernel(t_hbm, w_hbm, g_hbm, scale_ref, p_ref, rank_ref,
           t_buf, w_buf, g_buf, q_all, e_buf, max_buf, sum_buf, pos_buf, stat_own, stat_in,
           load_sem, gs_sem, gr_sem, ss_sem, sr_sem):
    me = lax.axis_index("ga")
    core = lax.rem(me, 2)
    pos = (me // 32, lax.rem(me // 8, 4), lax.rem(me // 2, 4))
    partner = me + 1 - 2 * core

    def peer(axis, k):
        there = list(pos)
        there[axis] = lax.rem(pos[axis] + k, 4)
        return device_of(there, core)

    loads = [pltpu.make_async_copy(src, dst, load_sem.at[i])
             for i, (src, dst) in enumerate(((t_hbm, t_buf), (w_hbm, w_buf), (g_hbm, g_buf)))]
    for load in loads:
        load.start()
    barrier = pltpu.get_barrier_semaphore()
    pl.semaphore_signal(barrier, inc=1, device_id=(partner,), device_id_type=MESH)
    for axis in range(3):
        for k in range(1, 4):
            pl.semaphore_signal(barrier, inc=1, device_id=(peer(axis, k),), device_id_type=MESH)

    mult = jnp.exp(jnp.full((1, 128), scale_ref[0], jnp.float32))
    coef = mult * (LOG2E / 2)

    loads[0].wait()
    loads[1].wait()
    u = jnp.dot(t_buf[...], w_buf[...], preferred_element_type=jnp.float32)
    unit = u / jnp.sqrt(jnp.sum(u * u, axis=1, keepdims=True))
    q_all[pos[0], pos[1], pos[2], core] = (unit * 2.0).astype(jnp.bfloat16)
    pl.semaphore_wait(barrier, 10)

    sends = []
    counter = [0]

    def view(fixed, c, col, ncol):
        idx = tuple(fixed[a] if a in fixed else slice(None) for a in range(3))
        return q_all.at[idx + (c, slice(None), pl.ds(col, ncol))]

    def send(fixed, col, ncol, slot, to):
        ref = view(fixed, core, col, ncol)
        copy = pltpu.make_async_remote_copy(ref, ref, gs_sem.at[slot], gr_sem.at[slot],
                                            device_id=(to,), device_id_type=MESH)
        copy.start()
        sends.append(copy)

    def recv(fixed, c, col, ncol, slot):
        ref = view(fixed, c, col, ncol)
        pltpu.make_async_remote_copy(ref, ref, gs_sem.at[slot], gr_sem.at[slot],
                                     device_id=(partner,), device_id_type=MESH).wait_recv()

    def fixed_at(order, phase, k=0):
        out = {}
        for i in range(phase, 3):
            a = order[i]
            out[a] = lax.rem(pos[a] + 4 - k, 4) if i == phase else pos[a]
        return out

    cross = []
    for phase in range(3):
        for r, (order, col, ncol) in enumerate(ROUTES):
            if phase > 0:
                for k in range(1, 4):
                    recv(fixed_at(order, phase - 1, k), core, col, ncol, r * 16 + (phase - 1) * 3 + k - 1)
            fixed = fixed_at(order, phase)
            for k in range(1, 4):
                send(fixed, col, ncol, r * 16 + phase * 3 + k - 1, peer(order[phase], k))
            if phase == 2:
                send(fixed, col, ncol, r * 16 + 9, partner)
                cross.append((fixed, col, ncol, r * 16 + 9))
    for k in range(1, 4):
        for r, (order, col, ncol) in enumerate(ROUTES):
            fixed = fixed_at(order, 2, k)
            recv(fixed, core, col, ncol, r * 16 + 6 + k - 1)
            send(fixed, col, ncol, r * 16 + 9 + k, partner)
            cross.append((fixed, col, ncol, r * 16 + 9 + k))
    for fixed, col, ncol, slot in cross:
        recv(fixed, 1 - core, col, ncol, slot)

    loads[2].wait()

    @pl.loop(0, 2048 // CHUNK)
    def _(i):
        rows = pl.multiple_of(i * CHUNK, CHUNK)
        q = q_all[i // 2, pl.ds(lax.rem(i, 2) * 2, 2)].reshape(CHUNK, 640)
        for n in range(8):
            e_buf[pl.ds(rows, CHUNK), n * 256:(n + 1) * 256] = lax.dot_general(
                q, g_buf[n * 256:(n + 1) * 256, :], (((1,), (1,)), ((), ())),
                preferred_element_type=jnp.float32)

        @pl.loop(0, CHUNK // 8, unroll=4)
        def _(j):
            r8 = pl.ds(pl.multiple_of(rows + j * 8, 8), 8)
            d = [e_buf[r8, c * 128:(c + 1) * 128] for c in range(16)]
            top = d
            while len(top) > 1:
                top = [jnp.maximum(a, b) for a, b in zip(top[::2], top[1::2])]
            top = top[0]
            total = None
            for c in range(15, -1, -1):
                e = jnp.exp2((d[c] - top) * coef)
                e_buf[r8, c * 128:(c + 1) * 128] = e
                total = e if total is None else total + e
                if c == 15:
                    weighted = total
                elif c > 0:
                    weighted = weighted + total
            max_buf[r8, :] = top
            sum_buf[r8, :] = total
            pos_buf[r8, :] = weighted

    base = (me * 2048).astype(jnp.float32)
    lane = lax.broadcasted_iota(jnp.int32, (128, 128), 0).astype(jnp.float32) + base

    @pl.loop(0, 16)
    def _(b):
        r128 = pl.ds(pl.multiple_of(b * 128, 128), 128)
        m_t = max_buf[r128, :].T
        z_t = sum_buf[r128, :].T
        w_t = pos_buf[r128, :].T
        m = jnp.max(m_t, axis=0, keepdims=True)
        scale = jnp.exp2((m_t - m) * coef)
        max_buf[r128, :] = m_t
        stat_own[0, pl.ds(b, 1), :] = m
        stat_own[1, pl.ds(b, 1), :] = jnp.sum(z_t * scale, axis=0, keepdims=True)
        stat_own[2, pl.ds(b, 1), :] = jnp.sum((z_t * lane + w_t * 128.0) * scale, axis=0, keepdims=True)

    def merge(parts):
        m = parts[0][0]
        for part in parts[1:]:
            m = jnp.maximum(m, part[0])
        z = s = None
        for pm, pz, ps in parts:
            f = jnp.exp2((pm - m) * coef)
            z = pz * f if z is None else z + pz * f
            s = ps * f if s is None else s + ps * f
        return m, z, s

    stage_axes = (None, X, Y, Z)
    for stage, axis in enumerate(stage_axes):
        if axis is None:
            here, others, n = core, [(partner, 0)], 2
        else:
            here, others, n = pos[axis], [(peer(axis, k), k - 1) for k in range(1, 4)], 4
        slots = stat_in.at[stage]
        slots[here] = stat_own[...]
        copies = []
        for to, k in others:
            copy = pltpu.make_async_remote_copy(
                stat_in.at[stage, here], stat_in.at[stage, here], ss_sem.at[stage, k], sr_sem.at[stage, k],
                device_id=(to,), device_id_type=MESH)
            copy.start()
            copies.append(copy)
            sends.append(copy)
        for copy in copies:
            copy.wait_recv()
        m, z, s = merge([tuple(slots[a, i] for i in range(3)) for a in range(n)])
        stat_own[0] = m
        stat_own[1] = z
        stat_own[2] = s
    rank_ref[...] = s / (z * 262144.0)

    @pl.loop(0, 16)
    def _(b):
        r128 = pl.ds(pl.multiple_of(b * 128, 128), 128)
        m = stat_own[0, pl.ds(b, 1), :]
        z = stat_own[1, pl.ds(b, 1), :]
        sum_buf[r128, :] = (jnp.exp2((max_buf[r128, :] - m) * coef) / z).T

    @pl.loop(0, 128, unroll=2)
    def _(j):
        r16 = pl.ds(pl.multiple_of(j * 16, 16), 16)
        f = sum_buf[r16, :]
        for c in range(16):
            p_ref[r16, c * 128:(c + 1) * 128] = (e_buf[r16, c * 128:(c + 1) * 128] * f).astype(jnp.bfloat16)

    for copy in sends:
        copy.wait_send()


def solution(mesh):
    def per_device(text_states, text_proj, gallery, logit_scale):
        p, rank = pl.pallas_call(
            kernel,
            out_shape=[pltpu.VMEM((2048, 2048), jnp.bfloat16), pltpu.VMEM((16, 128), jnp.float32)],
            in_specs=[pl.BlockSpec(memory_space=pltpu.HBM)] * 3 + [pl.BlockSpec(memory_space=pltpu.SMEM)],
            out_specs=[pl.BlockSpec(memory_space=pltpu.VMEM)] * 2,
            scratch_shapes=[
                pltpu.VMEM((16, 640), jnp.bfloat16),
                pltpu.VMEM((640, 640), jnp.bfloat16),
                pltpu.VMEM((2048, 640), jnp.bfloat16),
                pltpu.VMEM((4, 4, 4, 2, 16, 640), jnp.bfloat16),
                pltpu.VMEM((2048, 2048), jnp.float32),
                pltpu.VMEM((2048, 128), jnp.float32),
                pltpu.VMEM((2048, 128), jnp.float32),
                pltpu.VMEM((2048, 128), jnp.float32),
                pltpu.VMEM((3, 16, 128), jnp.float32),
                pltpu.VMEM((4, 4, 3, 16, 128), jnp.float32),
                pltpu.SemaphoreType.DMA((3,)),
                pltpu.SemaphoreType.DMA((48,)),
                pltpu.SemaphoreType.DMA((48,)),
                pltpu.SemaphoreType.DMA((4, 3)),
                pltpu.SemaphoreType.DMA((4, 3)),
            ],
            compiler_params=pltpu.CompilerParams(
                collective_id=0, has_side_effects=True, vmem_limit_bytes=40 * 2**20),
        )(text_states, text_proj, gallery, logit_scale)
        return p, rank.reshape(2048)

    return jax.shard_map(per_device, mesh=mesh,
                         in_specs=(P("ga", None), P(None, None), P("ga", None), P(None)),
                         out_specs=(P(None, "ga"), P(None)), check_vma=False)
```

```python
import jax
import jax.numpy as jnp
from jax import lax
from jax.experimental import pallas as pl
from jax.experimental.pallas import tpu as pltpu
from jax.sharding import PartitionSpec as P

MESH = pl.DeviceIdType.MESH
LOG2E = 1.4426950408889634
NEAR = (1, 3, 2)


def device_of(z, y, x, core):
    return ((z * 4 + y) * 4 + x) * 2 + core


def mod4(v):
    return lax.rem(v, 4)


def natural_order(v):
    row = lax.broadcasted_iota(jnp.int32, (16, 128), 0)
    lane = lax.broadcasted_iota(jnp.int32, (16, 128), 1)
    x, odd, r = lane // 32, lax.rem(lane // 16, 2), lax.rem(lane, 16)
    z, half = row // 4, lax.rem(row, 2) * 64

    def rows(pick):
        return jnp.concatenate([v[pick(i // 4, i % 4):pick(i // 4, i % 4) + 1] for i in range(16)], axis=0)

    out = jnp.take_along_axis(rows(lambda z, y: z * 2 + y // 2), half + x * 16 + r, axis=1)
    for at in range(4):
        part = jnp.take_along_axis(rows(lambda z, y: 8 + at * 2 + y // 2), half + z * 16 + r, axis=1)
        out = jnp.where((odd == 1) & (x == at), part, out)
    return out


def kernel(t_hbm, w_hbm, g_hbm, scale_ref, e_buf, maxt_buf, stat_own,
           t_buf, w_buf, g_buf, g_t, q_all, d_buf0, d_buf1, part_buf0, part_buf1, stat_in,
           load_sem, gs_sem, gr_sem, ss_sem, sr_sem):
    me = lax.axis_index("ga")
    core = lax.rem(me, 2)
    z, y, x = me // 32, mod4(me // 8), mod4(me // 2)
    partner = me + 1 - 2 * core
    first = x + core * (z - x)
    last = z + core * (x - z)

    def peer_first(k):
        f = mod4(first + k)
        return device_of(z + core * (f - z), y, f + core * (x - f), core)

    def peer_y(k):
        return device_of(z, mod4(y + k), x, core)

    def peer_last(k):
        f = mod4(last + k)
        return device_of(f + core * (z - f), y, x + core * (f - x), core)

    peers = {(n, k): f(k) for n, f in (("f", peer_first), ("y", peer_y), ("l", peer_last)) for k in (1, 2, 3)}

    loads = [pltpu.make_async_copy(src, dst, load_sem.at[i])
             for i, (src, dst) in enumerate(((t_hbm, t_buf), (w_hbm, w_buf), (g_hbm, g_buf)))]
    for load in loads:
        load.start()
    barrier = pltpu.get_barrier_semaphore()
    for to in (partner, *peers.values()):
        pl.semaphore_signal(barrier, inc=1, device_id=(to,), device_id_type=MESH)

    mult = jnp.exp(jnp.full((1, 128), scale_ref[0], jnp.float32))
    coef = mult * (LOG2E / 2)

    loads[0].wait()
    loads[1].wait()
    u = jnp.dot(t_buf[...], w_buf[...], preferred_element_type=jnp.float32)
    unit = u / jnp.sqrt(jnp.sum(u * u, axis=1, keepdims=True))
    q_all[core, last, y, first] = (unit * 2.0).astype(jnp.bfloat16)
    pl.semaphore_wait(barrier, 10)

    sends = []

    def send(ref, slot, to):
        copy = pltpu.make_async_remote_copy(ref, ref, gs_sem.at[slot], gr_sem.at[slot],
                                            device_id=(to,), device_id_type=MESH)
        copy.start()

    def recv(ref, slot):
        pltpu.make_async_remote_copy(ref, ref, gs_sem.at[slot], gr_sem.at[slot],
                                     device_id=(partner,), device_id_type=MESH).wait_recv()

    def line(c, k, j):
        at = last if c is core else first
        return q_all.at[c, mod4(at + 4 - k), mod4(y + 4 - j)]

    other = 1 - core

    def to_partner(k, j):
        send(line(core, k, j), 18 + k * 4 + j, partner)

    def from_partner(k):
        for j in range(4):
            recv(line(other, k, j), 18 + k * 4 + j)

    def to_last(j, k):
        send(line(core, 0, j), 6 + (k - 1) * 4 + j, peers["l", k])

    def from_last(k):
        for j in range(4):
            recv(line(core, k, j), 6 + (k - 1) * 4 + j)
            to_partner(k, j)

    def transpose(lo, hi):
        for n in range(lo, hi):
            g_t[:, n * 256:(n + 1) * 256] = g_buf[n * 256:(n + 1) * 256, :].T

    for k in NEAR:
        send(q_all.at[core, last, y, first], k - 1, peers["f", k])
    loads[2].wait()
    transpose(0, 4)
    for ref in (d_buf1, part_buf0, part_buf1):
        ref[...] = jnp.zeros_like(ref)
    for k in NEAR:
        recv(q_all.at[core, last, y, mod4(first + 4 - k)], k - 1)
    for k in NEAR:
        send(line(core, 0, 0), 2 + k, peers["y", k])
    for k in NEAR:
        to_last(0, k)
    to_partner(0, 0)
    transpose(4, 8)
    for j in NEAR:
        recv(line(core, 0, j), 2 + j)
        to_last(j, 1)
        to_last(j, 3)
        to_partner(0, j)
    for j in NEAR:
        to_last(j, 2)

    base = (me * 2048).astype(jnp.float32)
    lane = lax.broadcasted_iota(jnp.int32, (128, 128), 0).astype(jnp.float32) + base

    def plane_of(c, k):
        at = mod4((last if c is core else first) + 4 - k)
        return c, at, c * 4 + at

    def scores(plane, d_ref, n):
        c, at, _ = plane
        cols = slice(n * 512, (n + 1) * 512)
        d_ref[:, cols] = jnp.dot(q_all[c, at].reshape(256, 640), g_t[:, cols], preferred_element_type=jnp.float32)

    def softmax(plane, d_ref, part_ref, n):
        for j in range(n * 8, n * 8 + 8):
            r8 = pl.ds(j * 8, 8)
            to = pl.ds(pl.multiple_of(plane[2] * 256 + j * 8, 8), 8)
            d = [d_ref[r8, i * 128:(i + 1) * 128] for i in range(16)]
            top = d
            while len(top) > 1:
                top = [jnp.maximum(a, b) for a, b in zip(top[::2], top[1::2])]
            top = top[0]
            total = weighted = None
            for i in range(15, -1, -1):
                e = jnp.exp2((d[i] - top) * coef)
                e_buf[to, i * 128:(i + 1) * 128] = e
                total = e if total is None else total + e
                if i == 15:
                    weighted = total
                elif i > 0:
                    weighted = weighted + total
            part_ref[0, r8, :] = top
            part_ref[1, r8, :] = total
            part_ref[2, r8, :] = weighted

    def statistics(plane, part_ref, h):
        r128 = pl.ds(pl.multiple_of(plane[2] * 256 + h * 128, 128), 128)
        m_t, z_t, w_t = (part_ref[i, h * 128:(h + 1) * 128, :].T for i in range(3))
        m = jnp.max(m_t, axis=0, keepdims=True)
        scale = jnp.exp2((m_t - m) * coef)
        maxt_buf[r128, :] = m_t
        row = pl.ds(plane[2] * 2 + h, 1)
        stat_own[0, row, :] = m
        stat_own[1, row, :] = jnp.sum(z_t * scale, axis=0, keepdims=True)
        stat_own[2, row, :] = jnp.sum((z_t * lane + w_t * 128.0) * scale, axis=0, keepdims=True)

    def step(new, d_new, part_new, old, d_old, older, part_older):
        for n in range(4):
            if new is not None:
                scores(plane_of(*new), d_new, n)
            if n < 2:
                statistics(plane_of(*older), part_older, n)
            if old is not None:
                softmax(plane_of(*old), d_old, part_new, n)

    @pl.loop(0, 4)
    def _(i):
        k, before = (v + v // 2 - 2 * (v // 3) for v in (i, mod4(i + 3)))

        @pl.when(i == 1)
        def _():
            from_last(1)

        step((core, k), d_buf0, part_buf1, (other, before), d_buf1, (core, before), part_buf0)

        @pl.when(i == 1)
        def _():
            from_last(3)

        @pl.when(i == 2)
        def _():
            from_last(2)

        from_partner(k)
        step((other, k), d_buf1, part_buf0, (core, k), d_buf0, (other, before), part_buf1)

    step(None, None, part_buf1, (other, 2), d_buf1, (core, 2), part_buf0)
    step(None, None, None, None, None, (other, 2), part_buf1)

    def merge(parts):
        m = parts[0][0]
        for part in parts[1:]:
            m = jnp.maximum(m, part[0])
        total = rank = None
        for pm, pz, ps in parts:
            f = jnp.exp2((pm - m) * coef)
            total = pz * f if total is None else total + pz * f
            rank = ps * f if rank is None else rank + ps * f
        return m, total, rank

    for stage in range(4):
        if stage == 0:
            here, others, n = core, [(partner, 0)], 2
        else:
            here = (x, y, z)[stage - 1]
            others = [((device_of(z, y, mod4(x + k), core), device_of(z, mod4(y + k), x, core),
                        device_of(mod4(z + k), y, x, core))[stage - 1], k - 1) for k in NEAR]
            n = 4
        stat_in[stage, here] = stat_own[...]
        copies = []
        for to, k in others:
            copy = pltpu.make_async_remote_copy(
                stat_in.at[stage, here], stat_in.at[stage, here], ss_sem.at[stage, k], sr_sem.at[stage, k],
                device_id=(to,), device_id_type=MESH)
            copy.start()
            copies.append(copy)
            sends.append(copy)
        for copy in copies:
            copy.wait_recv()
        m, total, rank = merge([tuple(stat_in[stage, a, i] for i in range(3)) for a in range(n)])
        stat_own[0] = m
        stat_own[1] = total
        stat_own[2] = rank
    stat_own[2] = rank / (total * 262144.0)

    for copy in sends:
        copy.wait_send()
    for slot in range(34):
        ref = q_all.at[core, last, y, first] if slot < 3 else line(core, 0, 0)
        pltpu.make_async_remote_copy(ref, ref, gs_sem.at[slot], gr_sem.at[slot],
                                     device_id=(partner,), device_id_type=MESH).wait_send()


def scale_kernel(e_ref, maxt_ref, stat_ref, scale_ref, p_hbm, rank_hbm, p_buf, rank_buf, sem, rank_sem):
    coef = jnp.exp(jnp.full((1, 128), scale_ref[0], jnp.float32)) * (LOG2E / 2)
    rank_buf[...] = natural_order(stat_ref[2])
    rank = pltpu.make_async_copy(rank_buf, rank_hbm, rank_sem)
    rank.start()
    copies = [rank]
    for b in range(16):
        c, at, h = b // 8, (b // 2) % 4, b % 2
        m = stat_ref[0, b:b + 1, :]
        total = stat_ref[1, b:b + 1, :]
        factor = (jnp.exp2((maxt_ref[b * 128:(b + 1) * 128, :] - m) * coef) / total).T
        for line in range(2):
            for f in range(4):
                block = line * 4 + f
                r16 = slice(b * 128 + block * 16, b * 128 + block * 16 + 16)
                part = factor[block * 16:block * 16 + 16]
                for i in range(16):
                    p_buf[b, line, f, :, i * 128:(i + 1) * 128] = (e_ref[r16, i * 128:(i + 1) * 128] * part).astype(jnp.bfloat16)
            y = h * 2 + line
            to = p_hbm.at[at, y, :, 0] if c == 0 else p_hbm.at[:, y, at, 1]
            copy = pltpu.make_async_copy(p_buf.at[b, line], to, sem.at[b, line])
            copy.start()
            copies.append(copy)
    for copy in copies:
        copy.wait()


def solution(mesh):
    def per_device(text_states, text_proj, gallery, logit_scale):
        f32, bf16 = jnp.float32, jnp.bfloat16
        vmem = pl.BlockSpec(memory_space=pltpu.VMEM)
        smem = pl.BlockSpec(memory_space=pltpu.SMEM)
        e, maxt, stat = pl.pallas_call(
            kernel,
            out_shape=[pltpu.VMEM((2048, 2048), f32), pltpu.VMEM((2048, 128), f32), pltpu.VMEM((3, 16, 128), f32)],
            in_specs=[pl.BlockSpec(memory_space=pltpu.HBM)] * 3 + [smem],
            out_specs=[vmem] * 3,
            scratch_shapes=[
                pltpu.VMEM((16, 640), bf16),
                pltpu.VMEM((640, 640), bf16),
                pltpu.VMEM((2048, 640), bf16),
                pltpu.VMEM((640, 2048), bf16),
                pltpu.VMEM((2, 4, 4, 4, 16, 640), bf16),
                pltpu.VMEM((256, 2048), f32),
                pltpu.VMEM((256, 2048), f32),
                pltpu.VMEM((3, 256, 128), f32),
                pltpu.VMEM((3, 256, 128), f32),
                pltpu.VMEM((4, 4, 3, 16, 128), f32),
                pltpu.SemaphoreType.DMA((3,)),
                pltpu.SemaphoreType.DMA((34,)),
                pltpu.SemaphoreType.DMA((34,)),
                pltpu.SemaphoreType.DMA((4, 3)),
                pltpu.SemaphoreType.DMA((4, 3)),
            ],
            compiler_params=pltpu.CompilerParams(
                collective_id=0, has_side_effects=True, vmem_limit_bytes=36 * 2**20),
        )(*(pltpu.with_memory_space_constraint(v, pltpu.HBM) for v in (text_states, text_proj, gallery)), logit_scale)
        p, rank = pl.pallas_call(
            scale_kernel,
            out_shape=[jax.ShapeDtypeStruct((4, 4, 4, 2, 16, 2048), bf16), jax.ShapeDtypeStruct((16, 128), f32)],
            in_specs=[vmem] * 3 + [smem],
            out_specs=[pl.BlockSpec(memory_space=pltpu.HBM)] * 2,
            scratch_shapes=[
                pltpu.VMEM((16, 2, 4, 16, 2048), bf16),
                pltpu.VMEM((16, 128), f32),
                pltpu.SemaphoreType.DMA((16, 2)),
                pltpu.SemaphoreType.DMA,
            ],
            compiler_params=pltpu.CompilerParams(vmem_limit_bytes=36 * 2**20),
        )(e, maxt, stat, logit_scale)
        return p.reshape(2048, 2048), rank.reshape(2048)

    return jax.shard_map(per_device, mesh=mesh,
                         in_specs=(P("ga", None), P(None, None), P("ga", None), P(None)),
                         out_specs=(P(None, "ga"), P(None)), check_vma=False)
```
